256 devices in a mesh: ulysses: 16 (over z, x_hi), blk: 16 (over y, x_lo, core).
Axes of the slice: x: 4 (x_hi: 2, x_lo: 2; x = x_hi * 2 + x_lo), y: 4, z: 8, core: 2. Of those that a mesh axis runs over, the one named last changes fastest.
Arguments:
- queries: bfloat16 [16, 1024, 4096], P('blk', 'ulysses'), may hold values from -6 to 6
- key_rows: bfloat16 [16, 1024, 1024], P('blk', 'ulysses'), may hold values from -6 to 6
- value_rows: bfloat16 [16, 1024, 1024], P('blk', 'ulysses'), may hold values from -6 to 6
- tile_segment: int32 [128], replicated, may hold values from 0 to 31, never falling along the last dimension, each value on 1 to 8 neighbouring positions
Outputs:
- attended: bfloat16 [16, 1024, 4096], P('blk', 'ulysses')
The draws below stay inside these ranges and needn't reach their ends.
Inputs may be any that keep to these rules, and one draw needn't show every extreme that they name: `tile_segment`: segment numbers never fall along the sequence and each segment covers 1 to 8 tiles.
All inputs are finite; a program needn't handle non-finite values.
Results may differ from the reference program's by a relative error of at most 0.0045.
Values may be sent and summed in bfloat16 or wider, within the bound.
A program may use at most 64 MiB of HBM per device.

```python
import math
import jax
import jax.numpy as jnp
import numpy as np
from jax import lax

Q_HEADS = 32
KV_HEADS = 8
HEAD_DIM = 128
TILE = 128
BLOCK_LEN = 1024
BLOCKS = 16
TILES = 128


def draw_queries(key, part):
    seq_total = BLOCKS * BLOCK_LEN
    row_width = Q_HEADS * HEAD_DIM
    noise_key = jax.random.fold_in(key, 101)
    sample = jnp.clip(1.6 * jax.random.normal(noise_key, (seq_total, row_width), jnp.float32), -6.0, 6.0)
    return sample.reshape(BLOCKS, BLOCK_LEN, row_width).astype(jnp.bfloat16)


def draw_key_rows(key, part):
    seq_total = BLOCKS * BLOCK_LEN
    row_width = KV_HEADS * HEAD_DIM
    noise_key = jax.random.fold_in(key, 202)
    sample = jnp.clip(1.6 * jax.random.normal(noise_key, (seq_total, row_width), jnp.float32), -6.0, 6.0)
    return sample.reshape(BLOCKS, BLOCK_LEN, row_width).astype(jnp.bfloat16)


def block_levels(stream_key, extent, pieces, low, high):
    loudness = 1.0
    for axis_at, shards_of in pieces:
        draws = jax.random.uniform(jax.random.fold_in(jax.random.fold_in(stream_key, 6), axis_at), (shards_of,), jnp.float32, low / len(pieces), high / len(pieces))
        loudness = loudness * jnp.repeat(jnp.exp(draws), extent[axis_at] // shards_of).reshape((-1,) + (1,) * (len(extent) - 1 - axis_at))
    return loudness


def profile(amount, total, bound, skew):
    loads = [(1 << 20) // math.isqrt(standing ** skew) + 1 for standing in range(2, amount + 1)]
    rest, given = total - bound - (amount - 1), [1] * (amount - 1)
    while rest > 0:
        free = [i for i in range(amount - 1) if given[i] < bound]
        mass, budget = sum([loads[i] for i in free]), rest
        for i in free:
            more = min(bound - given[i], max(1, budget * loads[i] // mass), rest)
            given[i] = given[i] + more
            rest = rest - more
    return np.array([bound] + given)


def ragged_sizes(key, amount, total, reach, slope):
    if amount == 2:
        one = jax.random.randint(key, (), max(1, total - reach), min(reach, total - 1) + 1)
        return jnp.stack([one, total - one])
    sizes = jnp.asarray(profile(amount, total, reach, slope), jnp.int32)
    couples = (amount - 1) // 2
    giver, sink = sizes[1:1 + 2 * couples:2], sizes[2:2 + 2 * couples:2]
    margin = jnp.minimum(giver - 1, reach - sink)
    passed = jax.random.randint(jax.random.fold_in(key, 1), (couples,), 0, 1 << 20) % (margin + 1)
    sizes = sizes.at[1:1 + 2 * couples:2].set(giver - passed).at[2:2 + 2 * couples:2].set(sink + passed)
    return sizes[jax.random.permutation(jax.random.fold_in(key, 2), amount)]


def bell_draw(stream_key, extent, deviation, bound, shards=(), held_as=jnp.bfloat16):
    values = jax.random.normal(stream_key, extent, jnp.float32) * deviation
    if len(shards) > 0:
        values = block_levels(stream_key, extent, shards, -0.22, 0.18) * values
    return jnp.clip(values, min=-bound, max=bound).astype(held_as)


def setup_inputs(seed: int = 0) -> dict:
    key_of = jax.random.split(jax.random.key(seed), 5)
    queries = draw_queries(jax.random.fold_in(key_of[4], 71), 0)
    key_rows = draw_key_rows(jax.random.fold_in(key_of[4], 71), 0)
    value_rows = bell_draw(key_of[2], (BLOCKS, BLOCK_LEN, KV_HEADS * HEAD_DIM), 1.0, 6.0, ((0, 16), (1, 16)))
    tile_segment = jnp.searchsorted(jnp.cumsum(ragged_sizes(key_of[3], TILES // 4, TILES, 8, 0)), jnp.arange(TILES), side="right").astype(jnp.int32)
    return dict(queries=queries, key_rows=key_rows, value_rows=value_rows, tile_segment=tile_segment)


masked_score = -1.0e30


def visible(query_pos, query_seg, key_pos, key_seg):
    earlier = key_pos[None, :] <= query_pos[:, None]
    same_image = (key_seg[None, :] == query_seg[:, None]) & (query_seg[:, None] % 2 == 1)
    return earlier | same_image


def reference(queries, key_rows, value_rows, tile_segment):
    seq_total = queries.shape[0] * queries.shape[1]
    group_size = Q_HEADS // KV_HEADS
    query_flat = queries.reshape(seq_total, KV_HEADS, group_size, HEAD_DIM)
    key_flat = key_rows.reshape(seq_total, KV_HEADS, HEAD_DIM).astype(jnp.float32)
    value_flat = value_rows.reshape(seq_total, KV_HEADS, HEAD_DIM).astype(jnp.float32)
    positions = jnp.arange(seq_total, dtype=jnp.int32)
    segments = tile_segment[positions // TILE]
    block_rows = math.gcd(seq_total, 128)
    score_scale = HEAD_DIM ** -0.5

    def one_block(block_index):
        begin = (block_index * block_rows).astype(jnp.int32)
        query_block = lax.dynamic_slice_in_dim(query_flat, begin, block_rows, 0).astype(jnp.float32)
        query_pos = begin + jnp.arange(block_rows, dtype=jnp.int32)
        query_seg = lax.dynamic_slice_in_dim(segments, begin, block_rows, 0)
        allowed = visible(query_pos, query_seg, positions, segments)
        scores = jnp.einsum("qkgd,skd->kgqs", query_block, key_flat) * score_scale
        scores = jnp.where(allowed[None, None], scores, masked_score)
        new_max = jnp.max(scores, axis=3)
        weights = jnp.where(allowed[None, None], jnp.exp(scores - new_max[..., None]), 0.0)
        denominators = jnp.sum(weights, axis=3)
        rounded = lax.optimization_barrier(weights.astype(jnp.bfloat16))
        mixed = jnp.einsum("kgqs,skd->kgqd", rounded.astype(jnp.float32), value_flat) / denominators[..., None]
        return jnp.transpose(mixed, (2, 0, 1, 3)).reshape(block_rows, Q_HEADS * HEAD_DIM).astype(jnp.bfloat16)

    blocks_out = lax.map(one_block, jnp.arange(seq_total // block_rows, dtype=jnp.int32))
    return blocks_out.reshape(queries.shape)
```

```python
import math

import jax
import jax.numpy as jnp
from jax import lax
from jax.experimental import pallas as pl
from jax.experimental.pallas import tpu as pltpu
from jax.sharding import PartitionSpec as P

MESH = pl.DeviceIdType.MESH
D = 128
SCALE = D**-0.5 * math.log2(math.e)
MASKED = -1e30
ROWS = 64
ROUNDS = (
    ((0, 0), (1, 0), (3, 0), (0, 1), (0, 3)),
    ((2, 0), (0, 2), (1, 1), (1, 3), (3, 1), (3, 3)),
    ((2, 1), (2, 3), (1, 2), (3, 2), (2, 2)),
)


def attend(q, k, v, mask, rows, m_ref, l_ref, acc_ref):
    s = lax.dot_general(q, k, (((1,), (1,)), ((), ())), preferred_element_type=jnp.float32)
    if mask is not None:
        s = jnp.where(mask, s, MASKED)
    m_old = m_ref[rows, :]
    peak = jnp.max(s, axis=1, keepdims=True) * SCALE
    m_new = jnp.maximum(m_old, jnp.broadcast_to(peak, m_old.shape))
    alpha = jnp.exp2(m_old - m_new)
    p = jnp.exp2(s * SCALE - m_new[:, :1]).astype(jnp.bfloat16)
    both = jnp.concatenate([v, jnp.ones_like(v)], axis=1)
    o = lax.dot_general(p, both, (((1,), (0,)), ((), ())), preferred_element_type=jnp.float32)
    acc_ref[rows, :] = acc_ref[rows, :] * alpha + o[:, :D]
    l_ref[rows, :] = l_ref[rows, :] * alpha + o[:, D:]
    m_ref[rows, :] = m_new


def kernel(
    seg_ref, q_hbm, k_hbm, v_hbm, out_hbm,
    kv, qd, od, m_ref, l_ref, acc_ref,
    kv_send, kv_recv, q_send, q_recv, g_send, g_recv, c_send, c_recv, o_send, o_recv, here,
):
    u = lax.axis_index("ulysses")
    b = lax.axis_index("blk")
    z, xh = u // 2, u % 2
    y, xl, c = b // 4, (b // 2) % 2, b % 2
    x = 2 * xh + xl
    mirror = 15 - b

    def chip(xx, yy):
        return (2 * z + xx // 2, 4 * yy + 2 * (xx % 2) + c)

    def copy(src, dst, send, recv, device):
        return pltpu.make_async_remote_copy(
            src_ref=src, dst_ref=dst, send_sem=send, recv_sem=recv, device_id=device, device_id_type=MESH
        )

    plane = [(z + d) % 8 for d in range(8)]
    back = [(z + 8 - d) % 8 for d in range(8)]
    xs = [(x + d) % 4 for d in range(4)]
    ys = [(y + d) % 4 for d in range(4)]
    partner = (u, b + 1 - 2 * c)

    barrier = pltpu.get_barrier_semaphore()
    peers = [(2 * plane[d] + xh, b) for d in range(1, 8)] + [(2 * plane[d] + xh, mirror) for d in range(8)]
    peers += [chip(xs[1], y), chip(xs[3], y), chip(x, ys[1]), chip(x, ys[3]), partner]
    for peer in peers:
        pl.semaphore_signal(barrier, inc=1, device_id=peer, device_id_type=MESH)
    pl.semaphore_wait(barrier, len(peers))

    waits = []

    def kv_group(group, t):
        return kv.at[b, xh, group // 4, t, pl.ds(pl.multiple_of((group % 4) * ROWS, ROWS), ROWS)]

    def columns(ref, start, width):
        return ref.at[:, pl.ds(pl.multiple_of(start, width), width)]

    locals_ = []
    for t, ref in enumerate((k_hbm, v_hbm)):
        own = pltpu.make_async_copy(columns(ref, z * D, D), kv_group(z, t), here.at[t])
        own.start()
        locals_.append(own)
    order = (4, 3, 5, 2, 6, 1, 7)
    for d in order:
        for t, ref in enumerate((k_hbm, v_hbm)):
            go = copy(
                columns(ref, plane[d] * D, D), kv_group(z, t), kv_send.at[t, d], kv_recv.at[t, d],
                (2 * plane[d] + xh, b),
            )
            go.start()
            waits.append(go)
    q_own = pltpu.make_async_copy(columns(q_hbm, z * 4 * D, 2 * D), qd.at[0, z], here.at[2])
    q_own.start()
    for d in order + (0,):
        for job in range(2):
            if job == 0 and d == 0:
                continue
            go = copy(
                columns(q_hbm, plane[d] * 4 * D + job * 2 * D, 2 * D), qd.at[job, z],
                q_send.at[job, d], q_recv.at[job, d], (2 * plane[d] + xh, mirror if job else b),
            )
            go.start()
            waits.append(go)

    m_ref[...] = jnp.full(m_ref.shape, MASKED, jnp.float32)
    l_ref[...] = jnp.zeros(l_ref.shape, jnp.float32)
    acc_ref[...] = jnp.zeros(acc_ref.shape, jnp.float32)

    for own in locals_:
        own.wait()
    for d in order:
        for t, ref in enumerate((k_hbm, v_hbm)):
            copy(
                columns(ref, z * D, D), kv_group(back[d], t), kv_send.at[t, d], kv_recv.at[t, d], (u, mirror)
            ).wait_recv()

    def unit(h, p, s, core):
        xx, yy = (xs[p], ys[s]) if h == 0 else (xs[s], ys[p])
        return kv.at[4 * yy + 2 * (xx % 2) + core, xx // 2, h]

    def neighbour(h, axis, step):
        along_x = (axis == 0) == (h == 0)
        return chip(xs[step], y) if along_x else chip(x, ys[step])

    def send(h, p, s, axis, step, part):
        ref = unit(h, p, s, c)
        if part is not None:
            ref = ref.at[part]
        to_p, to_s = ((p - step) % 4, s) if axis == 0 else (p, (s - step) % 4)
        go = copy(
            ref, ref, g_send.at[h, p, s, 2 * axis + (step == 3)], g_recv.at[h, to_p, to_s, part or 0],
            neighbour(h, axis, step),
        )
        go.start()
        waits.append(go)

    def arrive(h, p, s):
        ref = unit(h, p, s, c)
        parts = (0, 1) if (s == 2 or (s == 0 and p == 2)) else (None,)
        for part in parts:
            got = ref if part is None else ref.at[part]
            copy(got, got, g_send.at[h, p, s, 0], g_recv.at[h, p, s, part or 0], partner).wait_recv()

    def relay(h, p, s):
        if s == 0:
            if p == 0:
                send(h, p, s, 0, 1, None)
                send(h, p, s, 0, 3, None)
            elif p == 1:
                send(h, p, s, 0, 3, 1)
            elif p == 3:
                send(h, p, s, 0, 1, 0)
            send(h, p, s, 1, 1, None)
            send(h, p, s, 1, 3, None)
        elif s == 1:
            send(h, p, s, 1, 3, 1)
        elif s == 3:
            send(h, p, s, 1, 1, 0)
        ref = unit(h, p, s, c)
        go = copy(ref, ref, c_send.at[h, p, s], c_recv.at[h, p, s], partner)
        go.start()
        waits.append(go)

    def from_partner(h, p, s):
        ref = unit(h, p, s, 1 - c)
        copy(ref, ref, c_send.at[h, p, s], c_recv.at[h, p, s], partner).wait_recv()

    early, late = jnp.minimum(b, mirror), jnp.maximum(b, mirror)
    job_block = (b, mirror)

    def q_tile(job, j):
        two = qd[job, pl.ds(2 * j, 2)].reshape(2 * ROWS, 2 * D)
        return jnp.concatenate([two[:, :D], two[:, D:]], axis=0)

    def tile_rows(job, j):
        return pl.ds(pl.multiple_of(job * 1024 + j * 256, 256), 256)

    def chunk(pair, half, t):
        return kv[pl.ds(2 * pair, 2), half, :, t].reshape(1024, D)

    def visible(block, j, pair, half, keys):
        at = lax.broadcasted_iota(jnp.int32, (1, keys), 1)
        tile = at >> 6
        k_pos = pair * 2048 + tile * 128 + half * ROWS + (at & 63)
        k_seg = jnp.zeros((1, keys), jnp.int32)
        for n in range(keys // ROWS):
            k_seg = jnp.where(tile == n, seg_ref[pair * 16 + n], k_seg)
        row = lax.broadcasted_iota(jnp.int32, (2 * ROWS, 1), 0)
        q_pos = block * 1024 + (2 * j + (row >> 6)) * 128 + xh * ROWS + (row & 63)
        q_seg = jnp.where(row < ROWS, seg_ref[block * 8 + 2 * j], seg_ref[block * 8 + 2 * j + 1])
        q_seg = jnp.where(q_seg % 2 == 1, q_seg, -1)
        one = (k_pos <= q_pos) | (k_seg == q_seg)
        return jnp.concatenate([one, one], axis=0)

    def full(jobs, pair, half):
        k, v = chunk(pair, half, 0), chunk(pair, half, 1)
        for job in jobs:
            for j in range(4):
                attend(q_tile(job, j), k, v, None, tile_rows(job, j), m_ref, l_ref, acc_ref)

    def masked(job, block, pair, half, keys):
        if keys == 1024:
            k, v = chunk(pair, half, 0), chunk(pair, half, 1)
        else:
            k, v = (kv[2 * pair, half, :, t].reshape(512, D) for t in range(2))
        for j in range(4):
            mask = visible(block, j, pair, half, keys)
            attend(q_tile(job, j), k, v, mask, tile_rows(job, j), m_ref, l_ref, acc_ref)

    def pick(values, i):
        out = jnp.int32(values[0])
        for n in range(1, len(values)):
            out = jnp.where(i == n, jnp.int32(values[n]), out)
        return out

    def compute(offsets):
        def one_chip(i, carry):
            xx = (x + pick([o[0] for o in offsets], i)) % 4
            yy = (y + pick([o[1] for o in offsets], i)) % 4
            pair, half = 2 * yy + xx % 2, xx // 2

            @pl.when(pair < early // 2)
            def _():
                full((0, 1), pair, half)

            @pl.when(pair >= early // 2)
            def _():
                def one_job(job, inner):
                    block = jnp.where(job == 0, job_block[0], job_block[1])

                    @pl.when(pair < block // 2)
                    def _():
                        full((job,), pair, half)

                    @pl.when(pair == block // 2)
                    def _():
                        masked(job, block, pair, half, 1024)

                    @pl.when((pair > block // 2) & (pair == (block + 1) // 2))
                    def _():
                        masked(job, block, pair, half, 512)

                    return inner

                lax.fori_loop(0, 2, one_job, 0)

            return carry

        lax.fori_loop(0, len(offsets), one_chip, 0)

    for h in range(2):
        relay(h, 0, 0)
    first = True
    stages = (
        ((1, 0), (3, 0), (0, 1), (0, 3)),
        ((2, 0), (1, 1), (1, 3), (3, 1), (3, 3), (0, 2)),
        ((2, 1), (2, 3), (1, 2), (3, 2)),
        ((2, 2),),
    )
    for number, stage in enumerate(stages):
        for p, s in stage:
            for h in range(2):
                arrive(h, p, s)
                relay(h, p, s)
        if number == 0:
            q_own.wait()
            for d in order + (0,):
                for job in range(2):
                    if job == 0 and d == 0:
                        continue
                    copy(
                        columns(q_hbm, z * 4 * D, 2 * D), qd.at[job, back[d]],
                        q_send.at[job, d], q_recv.at[job, d], partner,
                    ).wait_recv()
            for h in range(2):
                from_partner(h, 0, 0)
        for p, s in stage:
            for h in range(2):
                from_partner(h, p, s)
        if number < 2:
            compute(ROUNDS[number])
        elif number == 3:
            compute(ROUNDS[2])

    for job in range(2):
        for j in range(4):
            rows = tile_rows(job, j)
            o = (acc_ref[rows, :] / l_ref[rows, :]).astype(jnp.bfloat16)
            o = jnp.concatenate([o[: 2 * ROWS], o[2 * ROWS :]], axis=1)
            od[job, pl.ds(2 * j, 2)] = o.reshape(2, ROWS, 2 * D)
    for d in order + (0,):
        for job in range(2):
            if job == 0 and d == 0:
                continue
            go = copy(
                od.at[job, plane[d]], columns(out_hbm, z * 4 * D + job * 2 * D, 2 * D),
                o_send.at[job, d], o_recv.at[job, d], (2 * plane[d] + xh, mirror if job else b),
            )
            go.start()
            waits.append(go)
    o_own = pltpu.make_async_copy(od.at[0, z], columns(out_hbm, z * 4 * D, 2 * D), here.at[3])
    o_own.start()
    o_own.wait()
    for d in order + (0,):
        for job in range(2):
            if job == 0 and d == 0:
                continue
            copy(
                od.at[job, z], columns(out_hbm, back[d] * 4 * D + job * 2 * D, 2 * D),
                o_send.at[job, d], o_recv.at[job, d], partner,
            ).wait_recv()
    for go in waits:
        go.wait_send()


def local(queries, key_rows, value_rows, tile_segment):
    dma = pltpu.SemaphoreType.DMA
    hbm = pl.BlockSpec(memory_space=pl.ANY)
    out = pl.pallas_call(
        kernel,
        out_shape=jax.ShapeDtypeStruct(queries.shape[1:], jnp.bfloat16),
        in_specs=[pl.BlockSpec(memory_space=pltpu.SMEM), hbm, hbm, hbm],
        out_specs=hbm,
        scratch_shapes=[
            pltpu.VMEM((16, 2, 2, 2, 256, D), jnp.bfloat16),
            pltpu.VMEM((2, 8, ROWS, 2 * D), jnp.bfloat16),
            pltpu.VMEM((2, 8, ROWS, 2 * D), jnp.bfloat16),
            pltpu.VMEM((2048, D), jnp.float32),
            pltpu.VMEM((2048, D), jnp.float32),
            pltpu.VMEM((2048, D), jnp.float32),
            dma((2, 8)), dma((2, 8)),
            dma((2, 8)), dma((2, 8)),
            dma((2, 4, 4, 4)), dma((2, 4, 4, 2)),
            dma((2, 4, 4)), dma((2, 4, 4)),
            dma((2, 8)), dma((2, 8)),
            dma((4,)),
        ],
        compiler_params=pltpu.CompilerParams(
            collective_id=0, has_side_effects=True, vmem_limit_bytes=60 * 2**20
        ),
        name="attention",
    )(tile_segment, queries[0], key_rows[0], value_rows[0])
    return out[None]


def solution(mesh):
    return jax.shard_map(
        local,
        mesh=mesh,
        in_specs=(P("blk", "ulysses", None), P("blk", "ulysses", None), P("blk", "ulysses", None), P()),
        out_specs=P("blk", "ulysses", None),
        check_vma=False,
    )
```

```python
import math

import jax
import jax.numpy as jnp
from jax import lax
from jax.experimental import pallas as pl
from jax.experimental.pallas import tpu as pltpu
from jax.sharding import PartitionSpec as P

MESH = pl.DeviceIdType.MESH
D = 128
SCALE = D**-0.5 * math.log2(math.e)
MASKED = -1e30
ROWS = 64
PAIRS = ((1, 0), (0, 0), (1, 1), (1, 3), (0, 1), (0, 3), (1, 2), (0, 2))
STAGES = (
    ((1, 0), (3, 0), (0, 1), (0, 3)),
    ((2, 0), (1, 1), (1, 3), (3, 1), (3, 3), (0, 2)),
    ((2, 1), (2, 3), (1, 2), (3, 2)),
    ((2, 2),),
)


def dot(a, b, contract):
    return lax.dot_general(a, b, ((contract[0], contract[1]), ((), ())), preferred_element_type=jnp.float32)


def attend(tiles, k, v, m_ref, l_ref, acc_ref):
    both = jnp.concatenate([v, jnp.ones_like(v)], axis=1)
    scores = [dot(q, k, ((1,), (1,))) for q, _, _ in tiles]
    weights = []
    for s, (_, rows, mask) in zip(scores, tiles):
        if mask is not None:
            s = jnp.where(mask(), s, MASKED)
        m_old = m_ref[rows, :]
        peak = jnp.max(s, axis=1, keepdims=True) * SCALE
        m_new = jnp.maximum(m_old, jnp.broadcast_to(peak, m_old.shape))
        weights.append((jnp.exp2(s * SCALE - m_new[:, :1]).astype(jnp.bfloat16), jnp.exp2(m_old - m_new)))
        m_ref[rows, :] = m_new
    for (p, alpha), (_, rows, _) in zip(weights, tiles):
        o = dot(p, both, ((1,), (0,)))
        acc_ref[rows, :] = acc_ref[rows, :] * alpha + o[:, :D]
        l_ref[rows, :] = l_ref[rows, :] * alpha + o[:, D:]


def kernel(
    seg_ref, q_hbm, k_hbm, v_hbm, out_hbm,
    kv, qd, od, m_ref, l_ref, acc_ref,
    kv_send, kv_recv, q_send, q_recv, g_send, g_recv, c_send, c_recv, o_send, o_recv, here,
):
    u = lax.axis_index("ulysses")
    b = lax.axis_index("blk")
    z, xh = u // 2, u % 2
    y, xl, c = b // 4, (b // 2) % 2, b % 2
    x = 2 * xh + xl
    mirror = 15 - b

    def chip(xx, yy):
        return (2 * z + xx // 2, 4 * yy + 2 * (xx % 2) + c)

    def copy(src, dst, send, recv, device):
        return pltpu.make_async_remote_copy(
            src_ref=src, dst_ref=dst, send_sem=send, recv_sem=recv, device_id=device, device_id_type=MESH
        )

    plane = [(z + d) % 8 for d in range(8)]
    back = [(z + 8 - d) % 8 for d in range(8)]
    xs = [(x + d) % 4 for d in range(4)]
    ys = [(y + d) % 4 for d in range(4)]
    partner = (u, b + 1 - 2 * c)

    barrier = pltpu.get_barrier_semaphore()
    peers = [(2 * plane[d] + xh, b) for d in range(1, 8)] + [(2 * plane[d] + xh, mirror) for d in range(8)]
    peers += [chip(xs[1], y), chip(xs[3], y), chip(x, ys[1]), chip(x, ys[3]), partner]
    for peer in peers:
        pl.semaphore_signal(barrier, inc=1, device_id=peer, device_id_type=MESH)
    pl.semaphore_wait(barrier, len(peers))

    waits = []

    def kv_group(group, t):
        return kv.at[b, xh, group // 4, t, pl.ds(pl.multiple_of((group % 4) * ROWS, ROWS), ROWS)]

    def columns(ref, start, width):
        return ref.at[:, pl.ds(pl.multiple_of(start, width), width)]

    locals_ = []
    for t, ref in enumerate((k_hbm, v_hbm)):
        own = pltpu.make_async_copy(columns(ref, z * D, D), kv_group(z, t), here.at[t])
        own.start()
        locals_.append(own)
    order = (4, 3, 5, 2, 6, 1, 7)
    for d in order:
        for t, ref in enumerate((k_hbm, v_hbm)):
            go = copy(
                columns(ref, plane[d] * D, D), kv_group(z, t), kv_send.at[t, d], kv_recv.at[t, d],
                (2 * plane[d] + xh, b),
            )
            go.start()
            waits.append(go)
    q_own = pltpu.make_async_copy(columns(q_hbm, z * 4 * D, 2 * D), qd.at[0, z], here.at[2])
    q_own.start()
    for job in range(2):
        for d in order if job == 0 else order + (0,):
            go = copy(
                columns(q_hbm, plane[d] * 4 * D + job * 2 * D, 2 * D), qd.at[job, z],
                q_send.at[job, d], q_recv.at[job, d], (2 * plane[d] + xh, mirror if job else b),
            )
            go.start()
            waits.append(go)

    m_ref[...] = jnp.full(m_ref.shape, MASKED, jnp.float32)
    l_ref[...] = jnp.zeros(l_ref.shape, jnp.float32)
    acc_ref[...] = jnp.zeros(acc_ref.shape, jnp.float32)

    for own in locals_:
        own.wait()
    for d in order:
        for t, ref in enumerate((k_hbm, v_hbm)):
            copy(
                columns(ref, z * D, D), kv_group(back[d], t), kv_send.at[t, d], kv_recv.at[t, d], (u, mirror)
            ).wait_recv()

    def unit(h, p, s, core):
        xx, yy = (xs[p], ys[s]) if h == 0 else (xs[s], ys[p])
        return kv.at[4 * yy + 2 * (xx % 2) + core, xx // 2, h]

    def neighbour(h, axis, step):
        along_x = (axis == 0) == (h == 0)
        return chip(xs[step], y) if along_x else chip(x, ys[step])

    relays = []

    def hop(h, p, s, axis, step, part):
        ref = unit(h, p, s, c)
        if part is not None:
            ref = ref.at[part]
        to_p, to_s = ((p - step) % 4, s) if axis == 0 else (p, (s - step) % 4)
        return copy(
            ref, ref, g_send.at[h, p, s, 2 * axis + (step == 3)], g_recv.at[h, to_p, to_s, part or 0],
            neighbour(h, axis, step),
        )

    def send(*which):
        hop(*which).start()
        relays.append(which)

    def arrive(h, p, s):
        ref = unit(h, p, s, c)
        parts = (0, 1) if (s == 2 or (s == 0 and p == 2)) else (None,)
        for part in parts:
            got = ref if part is None else ref.at[part]
            copy(got, got, g_send.at[h, p, s, 0], g_recv.at[h, p, s, part or 0], partner).wait_recv()

    def relay(h, p, s):
        if s == 0:
            if p == 0:
                send(h, p, s, 0, 1, None)
                send(h, p, s, 0, 3, None)
            elif p == 1:
                send(h, p, s, 0, 3, 1)
            elif p == 3:
                send(h, p, s, 0, 1, 0)
            send(h, p, s, 1, 1, None)
            send(h, p, s, 1, 3, None)
        elif s == 1:
            send(h, p, s, 1, 3, 1)
        elif s == 3:
            send(h, p, s, 1, 1, 0)
        across(h, p, s, c).start()

    def across(h, p, s, core):
        ref = unit(h, p, s, core)
        return copy(ref, ref, c_send.at[h, p, s], c_recv.at[h, p, s], partner)

    def from_partner(h, p, s):
        across(h, p, s, 1 - c).wait_recv()

    early = jnp.where(b < 8, 0, 1)

    def block_of(job):
        return jnp.where(job == 0, b, mirror)

    def q_tile(job, j):
        two = qd[job, pl.ds(2 * j, 2)].reshape(2 * ROWS, 2 * D)
        return jnp.concatenate([two[:, :D], two[:, D:]], axis=0)

    def tile_rows(job, j):
        return pl.ds(pl.multiple_of(job * 1024 + j * 256, 256), 256)

    def masks(block, pair, keys):
        at = lax.broadcasted_iota(jnp.int32, (1, keys), 1)
        tile = ((at >> 10) << 3) + (((at >> 8) & 1) << 2) + ((at >> 6) & 3)
        k_pos = pair * 2048 + tile * 128 + ((at >> 9) & 1) * ROWS + (at & 63)
        k_seg = jnp.zeros((1, keys), jnp.int32)
        for n in range(keys // 128):
            k_seg = jnp.where(tile == n, seg_ref[pair * 16 + n], k_seg)

        def visible(j):
            row = lax.broadcasted_iota(jnp.int32, (2 * ROWS, 1), 0)
            q_pos = block * 1024 + (2 * j + (row >> 6)) * 128 + xh * ROWS + (row & 63)
            q_seg = jnp.where(row < ROWS, seg_ref[block * 8 + 2 * j], seg_ref[block * 8 + 2 * j + 1])
            q_seg = jnp.where(q_seg % 2 == 1, q_seg, -1)
            one = (k_pos <= q_pos) | (k_seg == q_seg)
            return jnp.concatenate([one, one], axis=0)

        return [lambda j=j: visible(j) for j in range(4)]

    def update(job, pair, blocks, mask):
        if blocks == 2:
            k, v = (kv[pl.ds(2 * pair, 2), :, :, t].reshape(2048, D) for t in range(2))
        else:
            k, v = (kv[2 * pair, :, :, t].reshape(1024, D) for t in range(2))
        tiles = [(q_tile(job, j), tile_rows(job, j), mask and mask[j]) for j in range(4)]
        attend(tiles, k, v, m_ref, l_ref, acc_ref)

    def attention(job, i):
        dx, dy = jnp.int32(PAIRS[0][0]), jnp.int32(PAIRS[0][1])
        for n in range(1, 8):
            dx, dy = jnp.where(i == n, PAIRS[n][0], dx), jnp.where(i == n, PAIRS[n][1], dy)
        pair = 2 * ((y + dy) % 4) + (x + dx) % 2
        block = block_of(job)

        @pl.when(pair < block // 2)
        def _():
            update(job, pair, 2, None)

        @pl.when(pair == block // 2)
        def _():
            update(job, pair, 2, masks(block, pair, 2048))

        @pl.when((pair > block // 2) & (pair == (block + 1) // 2))
        def _():
            update(job, pair, 1, masks(block, pair, 1024))

    def giving(job, d):
        return copy(
            od.at[job, plane[d]], columns(out_hbm, z * 4 * D + job * 2 * D, 2 * D),
            o_send.at[job, d], o_recv.at[job, d], (2 * plane[d] + xh, block_of(job)),
        )

    o_own = pltpu.make_async_copy(od.at[0, z], columns(out_hbm, z * 4 * D, 2 * D), here.at[3])

    def give(job):
        for j in range(4):
            rows = tile_rows(job, j)
            o = (acc_ref[rows, :] / l_ref[rows, :]).astype(jnp.bfloat16)
            o = jnp.concatenate([o[: 2 * ROWS], o[2 * ROWS :]], axis=1)
            od[job, pl.ds(2 * j, 2)] = o.reshape(2, ROWS, 2 * D)
        for d in order:
            giving(job, d).start()

        @pl.when(job == 0)
        def _():
            o_own.start()

        @pl.when(job == 1)
        def _():
            giving(job, 0).start()

    def gather(stage):
        for p, s in STAGES[stage]:
            for h in range(2):
                arrive(h, p, s)
                relay(h, p, s)

    def gathered(stage):
        for p, s in STAGES[stage]:
            for h in range(2):
                from_partner(h, p, s)

    def queries_of(job):
        if job == 0:
            q_own.wait()
        for d in order if job == 0 else order + (0,):
            copy(
                columns(q_hbm, z * 4 * D, 2 * D), qd.at[job, back[d]], q_send.at[job, d], q_recv.at[job, d], partner
            ).wait_recv()

    for h in range(2):
        relay(h, 0, 0)
    gather(0)
    queries_of(0)
    for h in range(2):
        from_partner(h, 0, 0)
    gathered(0)

    def step(n, carry):
        @pl.when(n == 1)
        def _():
            queries_of(1)

        @pl.when(n == 2)
        def _():
            gather(1)
            gathered(1)

        @pl.when(n == 5)
        def _():
            gather(2)

        @pl.when(n == 8)
        def _():
            gather(3)
            gathered(2)
            gathered(3)

        @pl.when(n == 12)
        def _():
            give(early)

        job = jnp.where(n < 8, n % 2, jnp.where(n < 12, early, 1 - early))
        attention(job, jnp.where(n < 8, n // 2, 4 + n % 4))
        return carry

    lax.fori_loop(0, 16, step, 0)
    give(1 - early)

    o_own.wait()
    for d in order + (0,):
        for job in range(2):
            if job == 0 and d == 0:
                continue
            copy(
                od.at[job, z], columns(out_hbm, back[d] * 4 * D + job * 2 * D, 2 * D),
                o_send.at[job, d], o_recv.at[job, d], partner,
            ).wait_recv()
            giving(job, d).wait_send()
    for go in waits:
        go.wait_send()
    for which in relays:
        hop(*which).wait_send()
    for stage in (((0, 0),),) + STAGES:
        for p, s in stage:
            for h in range(2):
                across(h, p, s, c).wait_send()


def local(queries, key_rows, value_rows, tile_segment):
    dma = pltpu.SemaphoreType.DMA
    hbm = pl.BlockSpec(memory_space=pl.ANY)
    out = pl.pallas_call(
        kernel,
        out_shape=jax.ShapeDtypeStruct(queries.shape[1:], jnp.bfloat16),
        in_specs=[pl.BlockSpec(memory_space=pltpu.SMEM), hbm, hbm, hbm],
        out_specs=hbm,
        scratch_shapes=[
            pltpu.VMEM((16, 2, 2, 2, 256, D), jnp.bfloat16),
            pltpu.VMEM((2, 8, ROWS, 2 * D), jnp.bfloat16),
            pltpu.VMEM((2, 8, ROWS, 2 * D), jnp.bfloat16),
            pltpu.VMEM((2048, D), jnp.float32),
            pltpu.VMEM((2048, D), jnp.float32),
            pltpu.VMEM((2048, D), jnp.float32),
            dma((2, 8)), dma((2, 8)),
            dma((2, 8)), dma((2, 8)),
            dma((2, 4, 4, 4)), dma((2, 4, 4, 2)),
            dma((2, 4, 4)), dma((2, 4, 4)),
            dma((2, 8)), dma((2, 8)),
            dma((4,)),
        ],
        compiler_params=pltpu.CompilerParams(
            collective_id=0, has_side_effects=True, vmem_limit_bytes=60 * 2**20
        ),
        name="attention",
    )(tile_segment, queries[0], key_rows[0], value_rows[0])
    return out[None]


def solution(mesh):
    return jax.shard_map(
        local,
        mesh=mesh,
        in_specs=(P("blk", "ulysses", None), P("blk", "ulysses", None), P("blk", "ulysses", None), P()),
        out_specs=P("blk", "ulysses", None),
        check_vma=False,
    )
```

```python
import math

import jax
import jax.numpy as jnp
from jax import lax
from jax.experimental import pallas as pl
from jax.experimental.pallas import tpu as pltpu
from jax.sharding import PartitionSpec as P

MESH = pl.DeviceIdType.MESH
D = 128
SCALE = D**-0.5 * math.log2(math.e)
MASKED = -1e30
ROWS = 64
PAIRS = ((1, 0), (0, 0), (1, 1), (1, 3), (0, 1), (0, 3), (1, 2), (0, 2))
STAGES = (
    ((1, 0), (3, 0), (0, 1), (0, 3)),
    ((2, 0), (1, 1), (1, 3), (3, 1), (3, 3), (0, 2)),
    ((2, 1), (2, 3), (1, 2), (3, 2)),
    ((2, 2),),
)


def dot(a, b, contract):
    return lax.dot_general(a, b, ((contract[0], contract[1]), ((), ())), preferred_element_type=jnp.float32)


def attend(tiles, k, v, m_ref, l_ref, acc_ref):
    both = jnp.concatenate([v, jnp.ones_like(v)], axis=1)
    scores = [dot(q, k, ((1,), (1,))) for q, _, _ in tiles]
    weights = []
    for s, (_, rows, mask) in zip(scores, tiles):
        if mask is not None:
            s = jnp.where(mask(), s, MASKED)
        m_old = m_ref[rows, :]
        peak = jnp.max(s, axis=1, keepdims=True) * SCALE
        m_new = jnp.maximum(m_old, jnp.broadcast_to(peak, m_old.shape))
        weights.append((jnp.exp2(s * SCALE - m_new[:, :1]).astype(jnp.bfloat16), jnp.exp2(m_old - m_new)))
        m_ref[rows, :] = m_new
    for (p, alpha), (_, rows, _) in zip(weights, tiles):
        o = dot(p, both, ((1,), (0,)))
        acc_ref[rows, :] = acc_ref[rows, :] * alpha + o[:, :D]
        l_ref[rows, :] = l_ref[rows, :] * alpha + o[:, D:]


def kernel(
    seg_ref, q_in, k_in, v_in, out_hbm,
    q_hbm, k_hbm, v_hbm, kv, qd, od, m_ref, l_ref, acc_ref,
    kv_send, kv_recv, q_send, q_recv, g_send, g_recv, c_send, c_recv, o_send, o_recv, here,
):
    u = lax.axis_index("ulysses")
    b = lax.axis_index("blk")
    z, xh = u // 2, u % 2
    y, xl, c = b // 4, (b // 2) % 2, b % 2
    x = 2 * xh + xl
    mirror = 15 - b

    def chip(xx, yy):
        return (2 * z + xx // 2, 4 * yy + 2 * (xx % 2) + c)

    def copy(src, dst, send, recv, device):
        return pltpu.make_async_remote_copy(
            src_ref=src, dst_ref=dst, send_sem=send, recv_sem=recv, device_id=device, device_id_type=MESH
        )

    plane = [(z + d) % 8 for d in range(8)]
    back = [(z + 8 - d) % 8 for d in range(8)]
    xs = [(x + d) % 4 for d in range(4)]
    ys = [(y + d) % 4 for d in range(4)]
    partner = (u, b + 1 - 2 * c)

    barrier = pltpu.get_barrier_semaphore()
    peers = [(2 * plane[d] + xh, b) for d in range(1, 8)] + [(2 * plane[d] + xh, mirror) for d in range(8)]
    peers += [chip(xs[1], y), chip(xs[3], y), chip(x, ys[1]), chip(x, ys[3]), partner]
    for peer in peers:
        pl.semaphore_signal(barrier, inc=1, device_id=peer, device_id_type=MESH)
    staged = []
    for n, (src, dst) in enumerate(((k_in, k_hbm), (v_in, v_hbm), (q_in, q_hbm))):
        stage = pltpu.make_async_copy(src, dst, here.at[n])
        stage.start()
        staged.append(stage)
    pl.semaphore_wait(barrier, len(peers))

    waits = []

    def kv_group(group, t):
        return kv.at[b, xh, group // 4, t, pl.ds(pl.multiple_of((group % 4) * ROWS, ROWS), ROWS)]

    def columns(ref, start, width):
        return ref.at[:, pl.ds(pl.multiple_of(start, width), width)]

    for stage in staged:
        stage.wait()
    locals_ = []
    for t, ref in enumerate((k_in, v_in)):
        own = pltpu.make_async_copy(columns(ref, z * D, D), kv_group(z, t), here.at[t])
        own.start()
        locals_.append(own)
    order = (4, 3, 5, 2, 6, 1, 7)
    for t, ref in enumerate((k_hbm, v_hbm)):
        for d in order:
            go = copy(
                columns(ref, plane[d] * D, D), kv_group(z, t), kv_send.at[t, d], kv_recv.at[t, d],
                (2 * plane[d] + xh, b),
            )
            go.start()
            waits.append(go)
    q_own = pltpu.make_async_copy(columns(q_in, z * 4 * D, 2 * D), qd.at[0, z], here.at[2])
    q_own.start()
    for job in range(2):
        for d in order if job == 0 else order + (0,):
            go = copy(
                columns(q_hbm, plane[d] * 4 * D + job * 2 * D, 2 * D), qd.at[job, z],
                q_send.at[job, d], q_recv.at[job, d], (2 * plane[d] + xh, mirror if job else b),
            )
            go.start()
            waits.append(go)

    m_ref[...] = jnp.full(m_ref.shape, MASKED, jnp.float32)
    l_ref[...] = jnp.zeros(l_ref.shape, jnp.float32)
    acc_ref[...] = jnp.zeros(acc_ref.shape, jnp.float32)

    def unit(h, p, s, core):
        xx, yy = (xs[p], ys[s]) if h == 0 else (xs[s], ys[p])
        return kv.at[4 * yy + 2 * (xx % 2) + core, xx // 2, h]

    def neighbour(h, axis, step):
        along_x = (axis == 0) == (h == 0)
        return chip(xs[step], y) if along_x else chip(x, ys[step])

    def wanted(h, p, s, core, y_to):
        x_from, y_from = (xs[p], ys[s]) if h == 0 else (xs[s], ys[p])
        return (y_from != 3) | (y_to == 0) | (y_to == 3) | ((core == 0) & (x_from % 2 == 0))

    def is_along_x(h, axis):
        return (axis == 0) == (h == 0)

    def hop(h, p, s, t, axis, step):
        ref = unit(h, p, s, c).at[t]
        to_p, to_s = ((p - step) % 4, s) if axis == 0 else (p, (s - step) % 4)
        return copy(
            ref, ref, g_send.at[h, p, s, 2 * axis + (step == 3), t], g_recv.at[h, to_p, to_s, t],
            neighbour(h, axis, step),
        )

    def goes(h, p, s, t, axis, step):
        along_x = is_along_x(h, axis)
        y_to = y if along_x else ys[step]
        yes = wanted(h, p, s, c, y) & wanted(h, p, s, c, y_to)
        at = p if axis == 0 else s
        if at and not along_x:
            turned = (ys[at] == 0) & (y_to == 2)
            if at == 3:
                yes = yes & jnp.logical_not(turned)
            elif t == 0:
                yes = yes & turned
        return yes

    def hops(h, p, s, t):
        found = []
        for axis in (0, 1) if s == 0 else (1,):
            at = p if axis == 0 else s
            if at in (0, 3) and (at == 0 or t == 0):
                found.append((h, p, s, t, axis, 1))
            if at == 0 or (at == 1 and (t == 1 or not is_along_x(h, axis))):
                found.append((h, p, s, t, axis, 3))
        return found

    def relay(h, p, s, t):
        for which in hops(h, p, s, t):

            @pl.when(goes(*which))
            def _():
                hop(*which).start()

        across(h, p, s, t, c).start()

    def arrive(h, p, s, t):
        ref = unit(h, p, s, c).at[t]
        copy(ref, ref, g_send.at[h, p, s, 0, t], g_recv.at[h, p, s, t], partner).wait_recv()

    def across(h, p, s, t, core):
        ref = unit(h, p, s, core).at[t]
        return copy(ref, ref, c_send.at[h, p, s, t], c_recv.at[h, p, s, t], partner)

    def from_partner(h, p, s):
        @pl.when(wanted(h, p, s, 1 - c, y))
        def _():
            for t in range(2):
                across(h, p, s, t, 1 - c).wait_recv()

    early = jnp.where(b < 8, 0, 1)

    def block_of(job):
        return jnp.where(job == 0, b, mirror)

    def q_tile(job, j):
        two = qd[job, pl.ds(2 * j, 2)].reshape(2 * ROWS, 2 * D)
        return jnp.concatenate([two[:, :D], two[:, D:]], axis=0)

    def tile_rows(job, j):
        return pl.ds(pl.multiple_of(job * 1024 + j * 256, 256), 256)

    def masks(block, pair, keys):
        at = lax.broadcasted_iota(jnp.int32, (1, keys), 1)
        tile = ((at >> 10) << 3) + (((at >> 8) & 1) << 2) + ((at >> 6) & 3)
        k_pos = pair * 2048 + tile * 128 + ((at >> 9) & 1) * ROWS + (at & 63)
        first = pair * 16
        start, image = jnp.maximum(first - 8, 0), jnp.full((1, keys), 1 << 20, jnp.int32)
        for n in range(-7, keys // 128):
            at_tile = jnp.maximum(first + n, 0)
            start = jnp.where(seg_ref[at_tile] == seg_ref[jnp.maximum(first + n - 1, 0)], start, at_tile)
            if n >= 0:
                image = jnp.where(tile == n, jnp.where(seg_ref[at_tile] % 2 == 1, start * 128, 1 << 20), image)
        k_from = jnp.minimum(k_pos, image)

        def visible(j):
            row = lax.broadcasted_iota(jnp.int32, (2 * ROWS, 1), 0)
            one = k_from <= block * 1024 + (2 * j + (row >> 6)) * 128 + xh * ROWS + (row & 63)
            return jnp.concatenate([one, one], axis=0)

        return [lambda j=j: visible(j) for j in range(4)]

    def update(job, pair, blocks, mask):
        if blocks == 2:
            k, v = (kv[pl.ds(2 * pair, 2), :, :, t].reshape(2048, D) for t in range(2))
        else:
            k, v = (kv[2 * pair, :, :, t].reshape(1024, D) for t in range(2))
        tiles = [(q_tile(job, j), tile_rows(job, j), mask and mask[j]) for j in range(4)]
        attend(tiles, k, v, m_ref, l_ref, acc_ref)

    def attention(job, i):
        dx, dy = jnp.int32(PAIRS[0][0]), jnp.int32(PAIRS[0][1])
        for n in range(1, 8):
            dx, dy = jnp.where(i == n, PAIRS[n][0], dx), jnp.where(i == n, PAIRS[n][1], dy)
        pair = 2 * ((y + dy) % 4) + (x + dx) % 2
        block = block_of(job)

        @pl.when(pair < block // 2)
        def _():
            update(job, pair, 2, None)

        @pl.when(pair == block // 2)
        def _():
            update(job, pair, 2, masks(block, pair, 2048))

        @pl.when((pair > block // 2) & (pair == (block + 1) // 2))
        def _():
            update(job, pair, 1, masks(block, pair, 1024))

    def giving(job, d):
        return copy(
            od.at[job, plane[d]], columns(out_hbm, z * 4 * D + job * 2 * D, 2 * D),
            o_send.at[job, d], o_recv.at[job, d], (2 * plane[d] + xh, block_of(job)),
        )

    o_own = pltpu.make_async_copy(od.at[0, z], columns(out_hbm, z * 4 * D, 2 * D), here.at[3])

    def give(job):
        for j in range(4):
            rows = tile_rows(job, j)
            o = (acc_ref[rows, :] / l_ref[rows, :]).astype(jnp.bfloat16)
            o = jnp.concatenate([o[: 2 * ROWS], o[2 * ROWS :]], axis=1)
            od[job, pl.ds(2 * j, 2)] = o.reshape(2, ROWS, 2 * D)
        for d in order:
            giving(job, d).start()

        @pl.when(job == 0)
        def _():
            o_own.start()

        @pl.when(job == 1)
        def _():
            giving(job, 0).start()

    def gather(stage):
        for t in range(2):
            for p, s in STAGES[stage]:
                for h in range(2):

                    @pl.when(wanted(h, p, s, c, y))
                    def _():
                        arrive(h, p, s, t)
                        relay(h, p, s, t)

    def gathered(stage):
        for p, s in STAGES[stage]:
            for h in range(2):
                from_partner(h, p, s)

    def queries_of(job):
        if job == 0:
            q_own.wait()
        for d in order if job == 0 else order + (0,):
            copy(
                columns(q_hbm, z * 4 * D, 2 * D), qd.at[job, back[d]], q_send.at[job, d], q_recv.at[job, d], partner
            ).wait_recv()

    for t, ref in enumerate((k_hbm, v_hbm)):
        locals_[t].wait()
        for d in order:
            copy(
                columns(ref, z * D, D), kv_group(back[d], t), kv_send.at[t, d], kv_recv.at[t, d], (u, mirror)
            ).wait_recv()
        for h in range(2):
            relay(h, 0, 0, t)
    gather(0)
    queries_of(0)
    for h in range(2):
        from_partner(h, 0, 0)
    gathered(0)

    def step(n, carry):
        @pl.when(n == 1)
        def _():
            queries_of(1)

        @pl.when(n == 2)
        def _():
            gather(1)
            gathered(1)

        @pl.when(n == 5)
        def _():
            gather(2)

        @pl.when(n == 8)
        def _():
            gather(3)
            gathered(2)
            gathered(3)

        @pl.when(n == 12)
        def _():
            give(early)

        job = jnp.where(n < 8, n % 2, jnp.where(n < 12, early, 1 - early))
        attention(job, jnp.where(n < 8, n // 2, 4 + n % 4))
        return carry

    lax.fori_loop(0, 16, step, 0)
    give(1 - early)

    for go in waits:
        go.wait_send()
    for stage in (((0, 0),),) + STAGES:
        for p, s in stage:
            for h in range(2):

                @pl.when(wanted(h, p, s, c, y))
                def _():
                    for t in range(2):
                        across(h, p, s, t, c).wait_send()
                        for which in hops(h, p, s, t):

                            @pl.when(goes(*which))
                            def _():
                                hop(*which).wait_send()

    o_own.wait()
    for d in order + (0,):
        for job in range(2):
            if job == 0 and d == 0:
                continue
            copy(
                od.at[job, z], columns(out_hbm, back[d] * 4 * D + job * 2 * D, 2 * D),
                o_send.at[job, d], o_recv.at[job, d], partner,
            ).wait_recv()
            giving(job, d).wait_send()


def local(queries, key_rows, value_rows, tile_segment):
    dma = pltpu.SemaphoreType.DMA
    hbm = pl.BlockSpec(memory_space=pl.ANY)
    out = pl.pallas_call(
        kernel,
        out_shape=jax.ShapeDtypeStruct(queries.shape[1:], jnp.bfloat16),
        in_specs=[pl.BlockSpec(memory_space=pltpu.SMEM), hbm, hbm, hbm],
        out_specs=hbm,
        scratch_shapes=[
            pltpu.VMEM(queries.shape[1:], jnp.bfloat16),
            pltpu.VMEM(key_rows.shape[1:], jnp.bfloat16),
            pltpu.VMEM(value_rows.shape[1:], jnp.bfloat16),
            pltpu.VMEM((16, 2, 2, 2, 256, D), jnp.bfloat16),
            pltpu.VMEM((2, 8, ROWS, 2 * D), jnp.bfloat16),
            pltpu.VMEM((2, 8, ROWS, 2 * D), jnp.bfloat16),
            pltpu.VMEM((2048, D), jnp.float32),
            pltpu.VMEM((2048, D), jnp.float32),
            pltpu.VMEM((2048, D), jnp.float32),
            dma((2, 8)), dma((2, 8)),
            dma((2, 8)), dma((2, 8)),
            dma((2, 4, 4, 4, 2)), dma((2, 4, 4, 2)),
            dma((2, 4, 4, 2)), dma((2, 4, 4, 2)),
            dma((2, 8)), dma((2, 8)),
            dma((4,)),
        ],
        compiler_params=pltpu.CompilerParams(
            collective_id=0, has_side_effects=True, vmem_limit_bytes=60 * 2**20
        ),
        name="attention",
    )(tile_segment, queries[0], key_rows[0], value_rows[0])
    return out[None]


def solution(mesh):
    return jax.shard_map(
        local,
        mesh=mesh,
        in_specs=(P("blk", "ulysses", None), P("blk", "ulysses", None), P("blk", "ulysses", None), P()),
        out_specs=P("blk", "ulysses", None),
        check_vma=False,
    )
```
